512 devices in a mesh: rows: 16 (over y, z_lo), cols: 32 (over z_hi, x, core).
Axes of the slice: x: 4, y: 4, z: 16 (z_hi: 4, z_lo: 4; z = z_hi * 4 + z_lo), core: 2. Of those that a mesh axis runs over, the one named last changes fastest.
Arguments:
- factor_u: float32 [16, 8192, 128], P('rows', 'cols'), may hold values from -2 to 2
- factor_v: float32 [32, 2048, 128], P('cols', 'rows'), may hold values from -2 to 2
- values: bfloat16 [16, 32, 32, 256, 256], P('rows', 'cols'), may hold values from -6 to 6
- mask_words: int32 [16, 32, 32, 16, 256], P('rows', 'cols'), may hold values from 0 to 65535, as said below
- tile_cols: int32 [16, 32, 32], P('rows', 'cols'), may hold values from 0 to 7
Outputs:
- new_u: float32 [16, 8192, 128], P('rows', 'cols')
- new_v: float32 [32, 2048, 128], P('cols', 'rows')
- loss: float32 [], replicated
The draws below stay inside these ranges and needn't reach their ends.
Inputs may be any that keep to these rules, and one draw needn't show every extreme that they name: `mask_words`: bit b of word w of a slot marks the entry in row 16 w + b of the tile.
All inputs are finite; a program needn't handle non-finite values.
Results may differ from the reference program's by a relative error of at most 0.02.
Values may be sent and summed in bfloat16 or wider, within the bound.
A program may use at most 64 MiB of HBM per device.

```python
import jax
import jax.numpy as jnp
from jax import lax

K = 128
TILE = 256
BAND_U = 8192
BAND_V = 2048
ROW_TILES = 32
COL_TILES = 8
ENTRIES = 1073741824
N_ROWS = 16
N_COLS = 32


def draw_mask_words(key, part):
    level_key = jax.random.fold_in(key, 11)
    ceiling_key = jax.random.fold_in(key, 12)
    bit_key = jax.random.fold_in(key, 13)
    levels = jax.random.randint(level_key, (N_ROWS, N_COLS, ROW_TILES), 0, 9)
    ceiling = jax.random.randint(ceiling_key, (N_ROWS, N_COLS, 1), 3, 10)
    levels = jnp.minimum(levels, ceiling)
    shifts = jnp.arange(16, dtype=jnp.int32)

    def draw_row(row_index):
        samples = jax.random.randint(jax.random.fold_in(bit_key, row_index), (N_COLS, ROW_TILES, TILE // 16, 16, TILE), 0, 8)
        bit_values = (samples < levels[row_index][:, :, None, None, None]).astype(jnp.int32)
        packed = jnp.sum(jnp.left_shift(bit_values, shifts[:, None]), axis=3)
        return packed.astype(jnp.int32)
    return lax.map(draw_row, jnp.arange(N_ROWS, dtype=jnp.int32))


def touch_ends(array, stream_key, least, top_value):
    dims = array.shape
    index_at = [jax.random.randint(jax.random.fold_in(stream_key, axis), (), 0, dims[axis]) for axis in range(len(dims))]
    array = array.at[tuple(index_at)].set(least)
    longest = dims.index(max(dims))
    index_at[longest] = (index_at[longest] + 1) % dims[longest]
    return array.at[tuple(index_at)].set(top_value)


def steps_of(key, shape, split, low, high):
    def one(dim, blocks):
        draws = jax.random.uniform(jax.random.fold_in(jax.random.fold_in(key, 6), dim), (blocks,), jnp.float32, low / len(split), high / len(split))
        return jnp.repeat(jnp.exp(draws), shape[dim] // blocks).reshape((-1,) + (1,) * (len(shape) - dim - 1))

    gain = one(*split[0])
    for cut in split[1:]:
        gain = gain * one(*cut)
    return gain


def gaussian(rng, shape, scale, bound, pieces=(), kind=jnp.bfloat16):
    result = scale * jax.random.normal(rng, shape, jnp.float32)
    if pieces:
        result = result * steps_of(rng, shape, pieces, -0.22, 0.18)
    return jnp.clip(result, -bound, bound).astype(kind)


def setup_inputs(seed: int = 0) -> dict:
    splits = jax.random.split(jax.random.key(seed), 6)
    return {
        "factor_u": gaussian(splits[0], (N_ROWS, BAND_U, K), 0.3, 2.0, ((0, 16), (1, 32)), jnp.float32),
        "factor_v": gaussian(splits[1], (N_COLS, BAND_V, K), 0.3, 2.0, ((0, 32), (1, 16)), jnp.float32),
        "values": gaussian(splits[2], (N_ROWS, N_COLS, ROW_TILES, TILE, TILE), 1.0, 6.0, ((0, 16), (1, 32))),
        "mask_words": draw_mask_words(jax.random.fold_in(splits[5], 71), 0),
        "tile_cols": touch_ends(jax.random.randint(splits[4], (N_ROWS, N_COLS, ROW_TILES), 0, COL_TILES), jax.random.fold_in(splits[4], 1), 0, COL_TILES - 1).astype(jnp.int32),
    }


step_rate = 0.01
ridge_weight = 0.1


def decode(mask_bits):
    shifts = jnp.arange(16, dtype=jnp.int32)
    bit_values = jnp.bitwise_and(jnp.right_shift(mask_bits[..., None, :], shifts[:, None]), 1)
    lead = mask_bits.shape[:-2]
    return bit_values.reshape(lead + (mask_bits.shape[-2] * 16, mask_bits.shape[-1])).astype(jnp.float32)


def rounded(array_in):
    return lax.optimization_barrier(array_in.astype(jnp.bfloat16)).astype(jnp.float32)


def device_terms(left_band, right_band, tile_values, mask_bits, column_ids):
    left_rows = left_band.reshape(-1, TILE, K).astype(jnp.float32)
    right_tiles = right_band.reshape(-1, TILE, K)
    right_rows = jnp.take(right_tiles, column_ids, axis=0).astype(jnp.float32)
    observed = decode(mask_bits)
    predicted = jnp.einsum("sik,sjk->sij", left_rows, right_rows, precision=lax.Precision.HIGHEST)
    residual = observed * (predicted - tile_values.astype(jnp.float32))
    resid_low = rounded(residual)
    grad_rows = jnp.einsum("sij,sjk->sik", resid_low, right_rows, precision=lax.Precision.HIGHEST)
    grad_cols = jnp.einsum("sij,sik->sjk", resid_low, left_rows, precision=lax.Precision.HIGHEST)
    col_sums = jax.ops.segment_sum(grad_cols, column_ids, num_segments=COL_TILES)
    squares = 0.5 * jnp.sum(residual * residual)
    return grad_rows.reshape(-1, K), col_sums.reshape(-1, K), squares


def reference(factor_u, factor_v, values, mask_words, tile_cols):
    u_low = factor_u.astype(jnp.bfloat16)
    v_low = factor_v.astype(jnp.bfloat16)

    def row_group(running, row_index):
        v_total, data_total = running

        def col_group(u_sum, col_index):
            grad_rows, col_sums, squares = device_terms(
                u_low[row_index], v_low[col_index], values[row_index, col_index],
                mask_words[row_index, col_index], tile_cols[row_index, col_index])
            return u_sum + rounded(grad_rows), (rounded(col_sums), squares)

        u_sum, outputs = lax.scan(col_group, jnp.zeros((BAND_U, K), jnp.float32),
                                  jnp.arange(N_COLS, dtype=jnp.int32))
        col_parts, square_parts = outputs
        return (v_total + col_parts, data_total + jnp.sum(square_parts)), u_sum

    initial = (jnp.zeros((N_COLS, BAND_V, K), jnp.float32), jnp.zeros((), jnp.float32))
    finals, grad_u = lax.scan(row_group, initial, jnp.arange(N_ROWS, dtype=jnp.int32))
    grad_v, data_total = finals
    penalty = 0.5 * ridge_weight * (jnp.sum(factor_u * factor_u) + jnp.sum(factor_v * factor_v))
    loss = (data_total + penalty) / ENTRIES
    new_u = factor_u - step_rate * (grad_u + ridge_weight * factor_u)
    new_v = factor_v - step_rate * (grad_v + ridge_weight * factor_v)
    return new_u, new_v, loss
```

```python
import jax
import jax.numpy as jnp
from jax import lax
from jax.experimental import pallas as pl
from jax.experimental.pallas import tpu as pltpu
from jax.sharding import PartitionSpec as P

F32 = jnp.float32
BF16 = jnp.bfloat16
STEP = 0.01
RIDGE = 0.1
MESH = pl.DeviceIdType.MESH
GROUP = 4


def wrap(i, n=4):
    return lax.rem(i + n, n)


class Place:
    def __init__(self):
        c = lax.axis_index("cols")
        r = lax.axis_index("rows")
        self.c, self.r = c, r
        self.k = lax.rem(c, 2)
        self.x = lax.rem(lax.div(c, 2), 4)
        self.zh = lax.div(c, 8)
        self.y = lax.div(r, 4)
        self.zl = lax.rem(r, 4)

    def col(self, dz=0, dx=0, dk=0):
        return wrap(self.zh + dz) * 8 + wrap(self.x + dx) * 2 + lax.rem(self.k + dk, 2)

    def row(self, dy=0, dl=0):
        return wrap(self.y + dy) * 4 + wrap(self.zl + dl)

    def dev(self, dz=0, dx=0, dk=0, dy=0, dl=0):
        if dy or dl:
            return {"rows": self.row(dy, dl)}
        return {"cols": self.col(dz, dx, dk)}


class Net:
    def __init__(self, send_sems, recv_sems):
        self.send_sems, self.recv_sems = send_sems, recv_sems
        self.ids, self.sent = {}, []

    def at(self, name):
        return self.ids.setdefault(name, len(self.ids))

    def send(self, name, src, dst, dev):
        i = self.at(name)
        copy = pltpu.make_async_remote_copy(
            src_ref=src, dst_ref=dst, send_sem=self.send_sems.at[i], recv_sem=self.recv_sems.at[i],
            device_id=dev, device_id_type=MESH)
        copy.start()
        self.sent.append(copy)

    def recv(self, name, ref, dev):
        i = self.at(name)
        pltpu.make_async_remote_copy(
            src_ref=ref, dst_ref=ref, send_sem=self.send_sems.at[i], recv_sem=self.recv_sems.at[i],
            device_id=dev, device_id_type=MESH).wait_recv()

    def finish(self):
        for copy in self.sent:
            copy.wait_send()


def greet(devs):
    barrier = pltpu.get_barrier_semaphore()
    for dev in devs:
        pl.semaphore_signal(barrier, inc=1, device_id=dev, device_id_type=MESH)
    pl.semaphore_wait(barrier, len(devs))


DZ = (0, -1, 1, 2)
N_GATHER = 80
N_REDUCE = 104


def gather_kernel(fu_ref, fv_ref, u_ref, v_ref, ridge_ref, send_sems, recv_sems):
    p = Place()
    net = Net(send_sems, recv_sems)
    u_ref[p.c] = fu_ref[...].astype(BF16)
    v_ref[p.r] = fv_ref[...].astype(BF16)
    greet([p.dev(dz=1), p.dev(dz=-1), p.dev(dx=1), p.dev(dx=-1), p.dev(dk=1),
           p.dev(dy=1), p.dev(dy=-1), p.dev(dl=1), p.dev(dl=2), p.dev(dl=3)])

    def ub(j, dx, h):
        return u_ref.at[p.col(DZ[j] if isinstance(j, int) else j[0], dx), pl.ds(h * 128, 128)]

    def vb(d, dy, h):
        return v_ref.at[p.row(dy, d), pl.ds(h * 64, 64)]

    class Ring:
        def __init__(self, tag, view, dev):
            self.tag, self.view, self.dev = tag, view, dev

        def put(self, j, h):
            for s in ((1, -1) if h == 0 else (-1, 1)):
                ref = self.view(j, 0, h)
                net.send((self.tag, j, s, h), ref, ref, self.dev(s))

        def forward(self, j):
            for s, h in ((1, 0), (-1, 1)):
                ref = self.view(j, -s, h)
                net.recv((self.tag, j, s, h), ref, self.dev(s))
                net.send((self.tag, j, s, "far"), ref, ref, self.dev(s))

        def finish(self, j, near=None, far=None):
            for s, h in ((1, 1), (-1, 0)):
                net.recv((self.tag, j, s, h), self.view(j, -s, h), self.dev(s))
            if near:
                near()
            for s, h in ((1, 0), (-1, 1)):
                net.recv((self.tag, j, s, "far"), self.view(j, 2, h), self.dev(s))
            if far:
                far()

    xr = Ring("x", ub, lambda s: p.dev(dx=s))
    yr = Ring("y", vb, lambda s: p.dev(dy=s))

    def twin(j, dx):
        ref = u_ref.at[p.col(DZ[j], dx)]
        net.send(("p", j, dx), ref, ref, p.dev(dk=1))

    def xfin(j):
        xr.finish(j, lambda: (twin(j, -1), twin(j, 1)), lambda: twin(j, 2))

    for s, h in ((1, 0), (-1, 1), (1, 1), (-1, 0)):
        ref = ub(0, 0, h)
        net.send(("z", s, h), ref, ref, p.dev(dz=s))
    for d in (1, 2, 3):
        ref = v_ref.at[p.r]
        net.send(("l", d), ref, ref, p.dev(dl=d))
    for h in (0, 1):
        xr.put(0, h)
    for h in (0, 1):
        yr.put(0, h)
    twin(0, 0)
    fu = fu_ref[...]
    fv = fv_ref[...]
    ridge_ref[...] = (0.5 * RIDGE) * (
        jnp.sum((fu * fu).reshape(32, 8, 128), axis=0) + jnp.sum((fv * fv).reshape(16, 8, 128), axis=0))
    xr.forward(0)
    yr.forward(0)
    for d in (1, 2, 3):
        net.recv(("l", d), v_ref.at[p.row(0, -d)], p.dev(dl=d))
        for h in (0, 1):
            yr.put(-d, h)
    xfin(0)

    def z_in(s, h, j):
        ref = ub(j, 0, h)
        net.recv(("z", s, h), ref, p.dev(dz=s))
        if (s, h) in ((1, 0), (-1, 1)):
            net.send(("z", s, "far"), ref, ref, p.dev(dz=s))
        xr.put(j, h)

    z_in(1, 0, 1)
    z_in(-1, 1, 2)
    for d in (1, 2, 3):
        yr.forward(-d)
    z_in(1, 1, 1)
    z_in(-1, 0, 2)
    twin(1, 0)
    twin(2, 0)
    xr.forward(1)
    xr.forward(2)
    for s, h in ((1, 0), (-1, 1)):
        net.recv(("z", s, "far"), ub(3, 0, h), p.dev(dz=s))
        xr.put(3, h)
    twin(3, 0)
    xfin(1)
    xfin(2)
    yr.finish(0)
    for d in (1, 2, 3):
        yr.finish(-d)
    xr.forward(3)
    xfin(3)
    for j in range(4):
        for dx in (0, -1, 1, 2):
            net.recv(("p", j, dx), u_ref.at[p.col(DZ[j], dx, 1)], p.dev(dk=1))
    net.finish()


def compute_kernel(ids_ref, u_ref, v_ref, vals_ref, mask_ref, ridge_ref, pu_ref, pv_ref, ls_ref, acc_v, acc_l):
    g = pl.program_id(0)

    @pl.when(g == 0)
    def _():
        acc_v[...] = jnp.zeros_like(acc_v)
        acc_l[...] = jnp.zeros_like(acc_l)

    probe = jnp.left_shift(1, lax.rem(lax.broadcasted_iota(jnp.int32, (16, 256), 0), 16))
    for i in range(GROUP):
        s = g * GROUP + i
        q = ids_ref[s]
        ut = u_ref[s]
        vt = v_ref[q]
        pred = lax.dot_general(ut, vt, (((1,), (1,)), ((), ())), preferred_element_type=F32)
        bits = jnp.concatenate(
            [jnp.bitwise_and(jnp.broadcast_to(mask_ref[i, w:w + 1, :], (16, 256)), probe) for w in range(16)], axis=0)
        res = jnp.where(bits != 0, pred - vals_ref[i].astype(F32), 0.0)
        acc_l[...] += jnp.sum((res * res).reshape(32, 8, 256), axis=0)
        low = res.astype(BF16)
        gu = jnp.dot(low, vt, preferred_element_type=F32)
        pu_ref[i % 2, 0, i // 2] = gu.astype(BF16)
        acc_v[q] += lax.dot_general(ut, low, (((0,), (0,)), ((), ())), preferred_element_type=F32)

    @pl.when(g == pl.num_programs(0) - 1)
    def _():
        for q in range(8):
            pv_ref[q] = acc_v[q].T.astype(BF16)
        half = acc_l[...]
        ls_ref[...] = 0.5 * (half[:, :128] + half[:, 128:]) + ridge_ref[...]


def reduce_kernel(entries, pu_ref, pv_ref, ls_ref, fu_ref, fv_ref, nu_ref, nv_ref, loss_ref,
                  pb, t, xb, xs, w, w0, zb, zs, yb, ys, wl, wl0, lb, le, ln, send_sems, recv_sems):
    p = Place()
    net = Net(send_sems, recv_sems)
    greet([p.dev(dk=1)] + [p.dev(dx=d) for d in (1, 2, 3)] + [p.dev(dz=d) for d in (1, 2, 3)]
          + [p.dev(dy=d) for d in (1, 2, 3)] + [p.dev(dl=d) for d in (1, 2, 3)])

    order = (3, 1, 2, 0)
    net.send(("lp",), ls_ref, le.at[0], p.dev(dk=1))
    for j in order:
        net.send(("p", j), pu_ref.at[1 - p.k, wrap(p.zh + DZ[j])], pb.at[j], p.dev(dk=1))

    def f(ref):
        return ref[...].astype(F32)

    class Ring:
        def __init__(self, tag, block, buf, mid, dev, half):
            self.tag, self.block, self.buf, self.mid, self.dev, self.half = tag, block, buf, mid, dev, half

        def part(self, j, i, h):
            return self.block(j, i).at[pl.ds(h * self.half, self.half)]

        def open(self, j):
            for s, h in ((1, 0), (-1, 1)):
                net.send((self.tag, j, s, "far"), self.part(j, 2, h), self.buf.at[j, h], self.dev(s))
            for s, h in ((1, 1), (-1, 0)):
                net.send((self.tag, j, s, "near"), self.part(j, s, h), self.buf.at[j, 2 + h], self.dev(s))

        def middle(self, j):
            for s, h in ((1, 0), (-1, 1)):
                net.recv((self.tag, j, s, "far"), self.buf.at[j, h], self.dev(s))
                self.mid[j, h] = (f(self.part(j, s, h)) + f(self.buf.at[j, h])).astype(BF16)
                net.send((self.tag, j, s, "mid"), self.mid.at[j, h], self.buf.at[j, 4 + h], self.dev(s))

        def close(self, j):
            out = []
            for s, h in ((1, 1), (-1, 0)):
                net.recv((self.tag, j, s, "near"), self.buf.at[j, 2 + h], self.dev(s))
            for s, h in ((1, 0), (-1, 1)):
                net.recv((self.tag, j, s, "mid"), self.buf.at[j, 4 + h], self.dev(s))
            for h in (0, 1):
                out.append(f(self.part(j, 0, h)) + f(self.buf.at[j, 2 + h]) + f(self.buf.at[j, 4 + h]))
            return out

    xr = Ring("x", lambda j, i: t.at[j, i % 4], xb, xs, lambda s: p.dev(dx=s), 128)
    yr = Ring("y", lambda d, i: pv_ref.at[p.row(i, d)], yb, ys, lambda s: p.dev(dy=s), 64)

    def s1(j):
        net.recv(("p", j), pb.at[j], p.dev(dk=1))
        zj = wrap(p.zh + DZ[j])
        for i in (2, 1, 3, 0):
            xa = wrap(p.x + i)
            t[j, i] = (pu_ref[p.k, zj, xa].astype(F32) + pb[j, xa].astype(F32)).astype(BF16)
        xr.open(j)

    def s3(j):
        a, b = xr.close(j)
        if j == 0:
            w0[0], w0[1] = a, b
        else:
            w[j, 0], w[j, 1] = a.astype(BF16), b.astype(BF16)
        if j == 3:
            net.send(("z", 1, "far"), w.at[3, 0], zb.at[0], p.dev(dz=1))
            net.send(("z", -1, "far"), w.at[3, 1], zb.at[1], p.dev(dz=-1))
        if j == 2:
            net.send(("z", 1, "near"), w.at[2, 1], zb.at[3], p.dev(dz=1))
        if j == 1:
            net.send(("z", -1, "near"), w.at[1, 0], zb.at[2], p.dev(dz=-1))

    steps = [0]

    def share(dev_of, mine):
        n = steps[0]
        steps[0] += 1
        for d in (1, 2, 3):
            net.send(("lo", n, d), mine, lb.at[n, d], dev_of(d))

    def shared(dev_of, mine):
        n = steps[0] - 1
        for d in (1, 2, 3):
            net.recv(("lo", n, d), lb.at[n, d], dev_of(d))
        total = (mine[...] + lb[n, 2]) + (lb[n, 1] + lb[n, 3])
        ln[n + 1] = total
        return ln.at[n + 1]

    xdev, ydev, ldev, zdev = (lambda d: p.dev(dx=d)), (lambda d: p.dev(dy=d)), (lambda d: p.dev(dl=d)), (lambda d: p.dev(dz=d))

    for d in (0, 1, 2, 3):
        yr.open(d)
    net.recv(("lp",), le.at[0], p.dev(dk=1))
    ln[0] = ls_ref[...] + le[0]
    part = ln.at[0]
    share(xdev, part)
    s1(3)
    s1(1)
    part = shared(xdev, part)
    share(ydev, part)
    for d in (2, 1, 3, 0):
        yr.middle(d)
    xr.middle(3)
    s1(2)
    s3(3)
    xr.middle(1)
    s1(0)
    part = shared(ydev, part)
    share(ldev, part)
    xr.middle(2)
    for d in (2, 1, 3):
        a, b = yr.close(d)
        wl[d, pl.ds(0, 64)], wl[d, pl.ds(64, 64)] = a.astype(BF16), b.astype(BF16)
        net.send(("l", d), wl.at[d], wl0.at[d], p.dev(dl=d))
    s3(1)
    s3(2)
    xr.middle(0)
    part = shared(ldev, part)
    share(zdev, part)
    for s, h, j in ((1, 0, 2), (-1, 1, 1)):
        net.recv(("z", s, "far"), zb.at[h], p.dev(dz=s))
        zs[h] = (f(w.at[j, h]) + f(zb.at[h])).astype(BF16)
        net.send(("z", s, "mid"), zs.at[h], zb.at[4 + h], p.dev(dz=s))
    s3(0)
    a, b = yr.close(0)
    for d in (1, 2, 3):
        net.recv(("l", d), wl0.at[d], p.dev(dl=d))
    for h, mine in ((0, a), (1, b)):
        rows = pl.ds(h * 64, 64)
        grad = mine + f(wl0.at[1, rows]) + f(wl0.at[2, rows]) + f(wl0.at[3, rows])
        old = fv_ref[rows]
        nv_ref[rows] = old - STEP * (grad + RIDGE * old)
    part = shared(zdev, part)
    loss_ref[0, 0] = jnp.sum(part[...]) * (1.0 / entries)
    for s, h in ((1, 1), (-1, 0)):
        net.recv(("z", s, "near"), zb.at[2 + h], p.dev(dz=s))
    for s, h in ((1, 0), (-1, 1)):
        net.recv(("z", s, "mid"), zb.at[4 + h], p.dev(dz=s))
        rows = pl.ds(h * 128, 128)
        grad = w0[h] + f(zb.at[2 + h]) + f(zb.at[4 + h])
        old = fu_ref[rows]
        nu_ref[rows] = old - STEP * (grad + RIDGE * old)
    net.finish()


def vmem():
    return pl.BlockSpec(memory_space=pltpu.VMEM)


def sems(n):
    return [pltpu.SemaphoreType.DMA((n,)), pltpu.SemaphoreType.DMA((n,))]


def per_device(factor_u, factor_v, values, mask_words, tile_cols):
    fu, fv = factor_u[0], factor_v[0]
    u_band, v_band, ridge = pl.pallas_call(
        gather_kernel,
        out_shape=(jax.ShapeDtypeStruct((32, 256, 128), BF16), jax.ShapeDtypeStruct((16, 128, 128), BF16),
                   jax.ShapeDtypeStruct((8, 128), F32)),
        in_specs=[vmem(), vmem()],
        out_specs=(vmem(), vmem(), vmem()),
        scratch_shapes=sems(N_GATHER),
        compiler_params=pltpu.CompilerParams(collective_id=0, has_side_effects=True),
        name="gather",
    )(fu, fv)
    pu, pv, ls = pl.pallas_call(
        compute_kernel,
        grid_spec=pltpu.PrefetchScalarGridSpec(
            num_scalar_prefetch=1,
            grid=(32 // GROUP,),
            in_specs=[
                vmem(),
                vmem(),
                pl.BlockSpec((GROUP, 256, 256), lambda g, ids: (g, 0, 0)),
                pl.BlockSpec((GROUP, 16, 256), lambda g, ids: (g, 0, 0)),
                vmem(),
            ],
            out_specs=(
                pl.BlockSpec((2, 1, 2, 256, 128), lambda g, ids: (0, lax.div(g, 2), lax.rem(g, 2), 0, 0)),
                vmem(),
                vmem(),
            ),
            scratch_shapes=[pltpu.VMEM((8, 128, 256), F32), pltpu.VMEM((8, 256), F32)],
        ),
        out_shape=(jax.ShapeDtypeStruct((2, 4, 4, 256, 128), BF16), jax.ShapeDtypeStruct((8, 256, 128), BF16),
                   jax.ShapeDtypeStruct((8, 128), F32)),
        compiler_params=pltpu.CompilerParams(dimension_semantics=("arbitrary",)),
        name="tiles",
    )(tile_cols[0, 0], u_band, v_band.reshape(8, 256, 128), values[0, 0], mask_words[0, 0], ridge)
    entries = lax.axis_size("rows") * lax.axis_size("cols") * 32 * 256 * 256
    new_u, new_v, loss = pl.pallas_call(
        lambda *refs: reduce_kernel(entries, *refs),
        out_shape=(jax.ShapeDtypeStruct((256, 128), F32), jax.ShapeDtypeStruct((128, 128), F32),
                   jax.ShapeDtypeStruct((1, 1), F32)),
        in_specs=[vmem()] * 5,
        out_specs=(vmem(), vmem(), pl.BlockSpec(memory_space=pltpu.SMEM)),
        scratch_shapes=[
            pltpu.VMEM((4, 4, 256, 128), BF16),
            pltpu.VMEM((4, 4, 256, 128), BF16),
            pltpu.VMEM((4, 6, 128, 128), BF16),
            pltpu.VMEM((4, 2, 128, 128), BF16),
            pltpu.VMEM((4, 2, 128, 128), BF16),
            pltpu.VMEM((2, 128, 128), F32),
            pltpu.VMEM((6, 128, 128), BF16),
            pltpu.VMEM((2, 128, 128), BF16),
            pltpu.VMEM((4, 6, 64, 128), BF16),
            pltpu.VMEM((4, 2, 64, 128), BF16),
            pltpu.VMEM((4, 128, 128), BF16),
            pltpu.VMEM((4, 128, 128), BF16),
            pltpu.VMEM((4, 4, 8, 128), F32),
            pltpu.VMEM((1, 8, 128), F32),
            pltpu.VMEM((5, 8, 128), F32),
            *sems(N_REDUCE),
        ],
        compiler_params=pltpu.CompilerParams(collective_id=1, has_side_effects=True),
        name="reduce",
    )(pu, pv.reshape(16, 128, 128), ls, fu, fv)
    return new_u[None], new_v[None], loss[0, 0]


def solution(mesh):
    return jax.shard_map(
        per_device,
        mesh=mesh,
        in_specs=(
            P("rows", "cols", None),
            P("cols", "rows", None),
            P("rows", "cols", None, None, None),
            P("rows", "cols", None, None, None),
            P("rows", "cols", None),
        ),
        out_specs=(P("rows", "cols", None), P("cols", "rows", None), P()),
        check_vma=False,
    )
```

```python
import jax
import jax.numpy as jnp
from jax import lax
from jax.experimental import pallas as pl
from jax.experimental.pallas import tpu as pltpu
from jax.sharding import PartitionSpec as P

F32 = jnp.float32
BF16 = jnp.bfloat16
STEP = 0.01
RIDGE = 0.1
MESH = pl.DeviceIdType.MESH


def wrap(i, n=4):
    return lax.rem(i + n, n)


class Place:
    def __init__(self):
        c = lax.axis_index("cols")
        r = lax.axis_index("rows")
        self.c, self.r = c, r
        self.k = lax.rem(c, 2)
        self.x = lax.rem(lax.div(c, 2), 4)
        self.zh = lax.div(c, 8)
        self.y = lax.div(r, 4)
        self.zl = lax.rem(r, 4)

    def col(self, dz=0, dx=0, dk=0):
        return wrap(self.zh + dz) * 8 + wrap(self.x + dx) * 2 + lax.rem(self.k + dk, 2)

    def row(self, dy=0, dl=0):
        return wrap(self.y + dy) * 4 + wrap(self.zl + dl)

    def dev(self, dz=0, dx=0, dk=0, dy=0, dl=0):
        if dy or dl:
            return {"rows": self.row(dy, dl)}
        return {"cols": self.col(dz, dx, dk)}


class Net:
    def __init__(self, send_sems, recv_sems):
        self.send_sems, self.recv_sems = send_sems, recv_sems
        self.ids, self.sent = {}, []

    def at(self, name):
        return self.ids.setdefault(name, len(self.ids))

    def send(self, name, src, dst, dev):
        i = self.at(name)
        copy = pltpu.make_async_remote_copy(
            src_ref=src, dst_ref=dst, send_sem=self.send_sems.at[i], recv_sem=self.recv_sems.at[i],
            device_id=dev, device_id_type=MESH)
        copy.start()
        self.sent.append(copy)

    def recv(self, name, ref, dev):
        i = self.at(name)
        pltpu.make_async_remote_copy(
            src_ref=ref, dst_ref=ref, send_sem=self.send_sems.at[i], recv_sem=self.recv_sems.at[i],
            device_id=dev, device_id_type=MESH).wait_recv()

    def finish(self):
        for copy in self.sent:
            copy.wait_send()


def greet(devs):
    barrier = pltpu.get_barrier_semaphore()
    for dev in devs:
        pl.semaphore_signal(barrier, inc=1, device_id=dev, device_id_type=MESH)
    pl.semaphore_wait(barrier, len(devs))


DZ = (0, -1, 1, 2)
N_COPIES = 184


def fused_kernel(entries, fu_ref, fv_ref, vals_hbm, mask_hbm, ids_ref, nu_ref, nv_ref, loss_ref,
                 u, v, vals, mask, prev, chain, pu, pv, ls, pb, t, xb, xs, w, w0, zb, zs, yb, ys, wl, wl0, lb, le, ln,
                 load_sems, send_sems, recv_sems):
    p = Place()
    net = Net(send_sems, recv_sems)

    def f(ref):
        return ref[...].astype(F32)

    loads = []
    for j in range(4):
        base = wrap(p.zh + DZ[j]) * 8
        for n, (far, near) in enumerate(((mask_hbm, mask), (vals_hbm, vals))):
            copy = pltpu.make_async_copy(far.at[pl.ds(base, 8)], near.at[pl.ds(base, 8)], load_sems.at[2 * j + n])
            copy.start()
            loads.append(copy)

    u[p.c] = fu_ref[...].astype(BF16)
    v[p.r] = fv_ref[...].astype(BF16)
    greet([p.dev(dk=1)] + [p.dev(dx=d) for d in (1, 2, 3)] + [p.dev(dz=d) for d in (1, 2, 3)]
          + [p.dev(dy=d) for d in (1, 2, 3)] + [p.dev(dl=d) for d in (1, 2, 3)])


    def ub(j, dx, h):
        return u.at[p.col(DZ[j], dx), pl.ds(h * 128, 128)]

    def vb(d, dy, h):
        return v.at[p.row(dy, d), pl.ds(h * 64, 64)]

    class Spread:
        def __init__(self, tag, view, dev):
            self.tag, self.view, self.dev = tag, view, dev

        def put(self, j, h):
            for s in ((1, -1) if h == 0 else (-1, 1)):
                ref = self.view(j, 0, h)
                net.send((self.tag, j, s, h), ref, ref, self.dev(s))

        def forward(self, j):
            for s, h in ((1, 0), (-1, 1)):
                ref = self.view(j, -s, h)
                net.recv((self.tag, j, s, h), ref, self.dev(s))
                net.send((self.tag, j, s, "hop"), ref, ref, self.dev(s))

        def finish(self, j, near=None, far=None):
            for s, h in ((1, 1), (-1, 0)):
                net.recv((self.tag, j, s, h), self.view(j, -s, h), self.dev(s))
            if near:
                near()
            for s, h in ((1, 0), (-1, 1)):
                net.recv((self.tag, j, s, "hop"), self.view(j, 2, h), self.dev(s))
            if far:
                far()

    xg = Spread("gx", ub, lambda s: p.dev(dx=s))
    yg = Spread("gy", vb, lambda s: p.dev(dy=s))

    def twin(j, dx):
        ref = u.at[p.col(DZ[j], dx)]
        net.send(("gp", j, dx), ref, ref, p.dev(dk=1))

    def xfin(j):
        xg.finish(j, lambda: (twin(j, -1), twin(j, 1)), lambda: twin(j, 2))

    def z_in(s, h, j):
        ref = ub(j, 0, h)
        net.recv(("gz", s, h), ref, p.dev(dz=s))
        if (s, h) in ((1, 0), (-1, 1)):
            net.send(("gz", s, "hop"), ref, ref, p.dev(dz=s))
        xg.put(j, h)

    def z_far():
        for s, h in ((1, 0), (-1, 1)):
            net.recv(("gz", s, "hop"), ub(3, 0, h), p.dev(dz=s))
            xg.put(3, h)
        twin(3, 0)


    order = (0, 1, 2, 3)
    probe = jnp.left_shift(1, lax.rem(lax.broadcasted_iota(jnp.int32, (16, 256), 0), 16))

    def links():
        last = [jnp.int32(-1)] * 8
        for n in range(32):
            j, m = order[n // 8], n % 8
            q = ids_ref[p.col(DZ[j], m // 2, m % 2)]
            before = jnp.int32(-1)
            for tile in range(8):
                hit = q == tile
                before = jnp.where(hit, last[tile], before)
                last[tile] = jnp.where(hit, n, last[tile])
            prev[n] = before
        for tile in range(8):
            prev[32 + tile] = last[tile]

    def linked(n):
        return jnp.where(n >= 0, chain[jnp.maximum(n, 0)], 0.0)

    def work(j, squares):
        for dx in (0, -1, 1, 2):
            net.recv(("gp", j, dx), u.at[p.col(DZ[j], dx, 1)], p.dev(dk=1))
        loads[2 * j].wait()
        loads[2 * j + 1].wait()
        zj = wrap(p.zh + DZ[j])
        first = order.index(j) * 8

        def slot(m, squares):
            i, kk = lax.div(m, 2), lax.rem(m, 2)
            s = zj * 8 + lax.rem(p.x + i, 4) * 2 + lax.rem(p.k + kk, 2)
            q = ids_ref[s]
            ut = u[s]
            vt = v[pl.ds(2 * q, 2)].reshape(256, 128)
            pred = lax.dot_general(ut, vt, (((1,), (1,)), ((), ())), preferred_element_type=F32)
            bits = jnp.concatenate(
                [jnp.bitwise_and(jnp.broadcast_to(mask[s, b:b + 1, :], (16, 256)), probe) for b in range(16)], axis=0)
            res = jnp.where(bits != 0, pred - vals[s].astype(F32), 0.0)
            low = res.astype(BF16)
            pu[j, kk, i] = jnp.dot(low, vt, preferred_element_type=F32).astype(BF16)
            chain[first + m] = linked(prev[first + m]) + lax.dot_general(
                ut, low, (((0,), (0,)), ((), ())), preferred_element_type=F32)
            return squares + jnp.sum((res * res).reshape(32, 8, 256), axis=0)

        squares = lax.fori_loop(0, 8, slot, squares)
        net.send(("p", j), pu.at[j, 1], pb.at[j], p.dev(dk=1))
        return squares


    class Ring:
        def __init__(self, tag, block, buf, mid, dev, half):
            self.tag, self.block, self.buf, self.mid, self.dev, self.half = tag, block, buf, mid, dev, half

        def part(self, j, i, h):
            return self.block(j, i).at[pl.ds(h * self.half, self.half)]

        def open(self, j):
            for s, h in ((1, 0), (-1, 1)):
                net.send((self.tag, j, s, "far"), self.part(j, 2, h), self.buf.at[j, h], self.dev(s))
            for s, h in ((1, 1), (-1, 0)):
                net.send((self.tag, j, s, "near"), self.part(j, s, h), self.buf.at[j, 2 + h], self.dev(s))

        def middle(self, j):
            for s, h in ((1, 0), (-1, 1)):
                net.recv((self.tag, j, s, "far"), self.buf.at[j, h], self.dev(s))
                self.mid[j, h] = (f(self.part(j, s, h)) + f(self.buf.at[j, h])).astype(BF16)
                net.send((self.tag, j, s, "mid"), self.mid.at[j, h], self.buf.at[j, 4 + h], self.dev(s))

        def close(self, j):
            out = []
            for s, h in ((1, 1), (-1, 0)):
                net.recv((self.tag, j, s, "near"), self.buf.at[j, 2 + h], self.dev(s))
            for s, h in ((1, 0), (-1, 1)):
                net.recv((self.tag, j, s, "mid"), self.buf.at[j, 4 + h], self.dev(s))
            for h in (0, 1):
                out.append(f(self.part(j, 0, h)) + f(self.buf.at[j, 2 + h]) + f(self.buf.at[j, 4 + h]))
            return out

    xr = Ring("x", lambda j, i: t.at[j, i % 4], xb, xs, lambda s: p.dev(dx=s), 128)
    yr = Ring("y", lambda d, i: pv.at[p.row(i, d)], yb, ys, lambda s: p.dev(dy=s), 64)

    def s1(j):
        net.recv(("p", j), pb.at[j], p.dev(dk=1))
        for i in (2, 1, 3, 0):
            t[j, i] = (pu[j, 0, i].astype(F32) + pb[j, i].astype(F32)).astype(BF16)
        xr.open(j)

    def s3(j):
        a, b = xr.close(j)
        if j == 0:
            w0[0], w0[1] = a, b
        else:
            w[j, 0], w[j, 1] = a.astype(BF16), b.astype(BF16)
        if j == 3:
            net.send(("z", 1, "far"), w.at[3, 0], zb.at[0], p.dev(dz=1))
            net.send(("z", -1, "far"), w.at[3, 1], zb.at[1], p.dev(dz=-1))
        if j == 2:
            net.send(("z", 1, "near"), w.at[2, 1], zb.at[3], p.dev(dz=1))
        if j == 1:
            net.send(("z", -1, "near"), w.at[1, 0], zb.at[2], p.dev(dz=-1))

    def share(n, dev_of):
        for d in (1, 2, 3):
            net.send(("lo", n, d), ln.at[n], lb.at[n, d], dev_of(d))

    def shared(n, dev_of):
        for d in (1, 2, 3):
            net.recv(("lo", n, d), lb.at[n, d], dev_of(d))
        ln[n + 1] = (ln[n] + lb[n, 2]) + (lb[n, 1] + lb[n, 3])

    axes = (lambda d: p.dev(dx=d), lambda d: p.dev(dy=d), lambda d: p.dev(dl=d), lambda d: p.dev(dz=d))


    for s, h in ((1, 0), (-1, 1), (1, 1), (-1, 0)):
        ref = ub(0, 0, h)
        net.send(("gz", s, h), ref, ref, p.dev(dz=s))
    for d in (1, 2, 3):
        ref = v.at[p.r]
        net.send(("gl", d), ref, ref, p.dev(dl=d))
    for h in (0, 1):
        xg.put(0, h)
    for h in (0, 1):
        yg.put(0, h)
    twin(0, 0)
    fu = fu_ref[...]
    fv = fv_ref[...]
    ridge = (0.5 * RIDGE) * (
        jnp.sum((fu * fu).reshape(32, 8, 128), axis=0) + jnp.sum((fv * fv).reshape(16, 8, 128), axis=0))
    links()
    xg.forward(0)
    yg.forward(0)
    for d in (1, 2, 3):
        net.recv(("gl", d), v.at[p.row(0, -d)], p.dev(dl=d))
        for h in (0, 1):
            yg.put(-d, h)
    xfin(0)
    z_in(1, 0, 1)
    z_in(-1, 1, 2)
    for d in (1, 2, 3):
        yg.forward(-d)
    z_in(1, 1, 1)
    z_in(-1, 0, 2)
    twin(1, 0)
    twin(2, 0)
    xg.forward(1)
    xg.forward(2)
    yg.finish(0)
    for d in (1, 2, 3):
        yg.finish(-d)
    squares = jnp.zeros((8, 256), F32)
    squares = work(0, squares)
    z_far()
    xfin(1)
    xfin(2)
    squares = work(1, squares)
    xg.forward(3)
    squares = work(2, squares)
    xfin(3)
    s1(0)
    s1(1)
    squares = work(3, squares)
    ls[...] = 0.5 * (squares[:, :128] + squares[:, 128:]) + ridge
    net.send(("lp",), ls, le.at[0], p.dev(dk=1))
    xr.middle(0)
    xr.middle(1)
    s1(2)
    for q in range(8):
        pv[pl.ds(2 * q, 2)] = linked(prev[32 + q]).T.astype(BF16).reshape(2, 128, 128)
    for d in (0, 1, 2, 3):
        yr.open(d)
    s1(3)
    s3(1)
    xr.middle(2)
    net.recv(("lp",), le.at[0], p.dev(dk=1))
    ln[0] = ls[...] + le[0]
    share(0, axes[0])
    for d in (2, 1, 3, 0):
        yr.middle(d)
    xr.middle(3)
    s3(2)
    shared(0, axes[0])
    share(1, axes[1])
    s3(3)
    for d in (2, 1, 3):
        a, b = yr.close(d)
        wl[d, pl.ds(0, 64)], wl[d, pl.ds(64, 64)] = a.astype(BF16), b.astype(BF16)
        net.send(("l", d), wl.at[d], wl0.at[d], p.dev(dl=d))
    shared(1, axes[1])
    share(2, axes[2])
    s3(0)
    shared(2, axes[2])
    share(3, axes[3])
    for s, h, j in ((1, 0, 2), (-1, 1, 1)):
        net.recv(("z", s, "far"), zb.at[h], p.dev(dz=s))
        zs[h] = (f(w.at[j, h]) + f(zb.at[h])).astype(BF16)
        net.send(("z", s, "mid"), zs.at[h], zb.at[4 + h], p.dev(dz=s))
    a, b = yr.close(0)
    for d in (1, 2, 3):
        net.recv(("l", d), wl0.at[d], p.dev(dl=d))
    for h, mine in ((0, a), (1, b)):
        rows = pl.ds(h * 64, 64)
        grad = mine + f(wl0.at[1, rows]) + f(wl0.at[2, rows]) + f(wl0.at[3, rows])
        old = fv_ref[rows]
        nv_ref[rows] = old - STEP * (grad + RIDGE * old)
    shared(3, axes[3])
    loss_ref[0, 0] = jnp.sum(ln[4]) * (1.0 / entries)
    for s, h in ((1, 1), (-1, 0)):
        net.recv(("z", s, "near"), zb.at[2 + h], p.dev(dz=s))
    for s, h in ((1, 0), (-1, 1)):
        net.recv(("z", s, "mid"), zb.at[4 + h], p.dev(dz=s))
        rows = pl.ds(h * 128, 128)
        grad = w0[h] + f(zb.at[2 + h]) + f(zb.at[4 + h])
        old = fu_ref[rows]
        nu_ref[rows] = old - STEP * (grad + RIDGE * old)
    net.finish()


def vmem():
    return pl.BlockSpec(memory_space=pltpu.VMEM)


def per_device(factor_u, factor_v, values, mask_words, tile_cols):
    entries = lax.axis_size("rows") * lax.axis_size("cols") * 32 * 256 * 256
    far = pl.BlockSpec(memory_space=pltpu.HBM)
    near = pl.BlockSpec(memory_space=pltpu.SMEM)

    def low(*shape):
        return pltpu.VMEM(shape, BF16)

    def full(*shape):
        return pltpu.VMEM(shape, F32)

    new_u, new_v, loss = pl.pallas_call(
        lambda *refs: fused_kernel(entries, *refs),
        out_shape=(jax.ShapeDtypeStruct((256, 128), F32), jax.ShapeDtypeStruct((128, 128), F32),
                   jax.ShapeDtypeStruct((1, 1), F32)),
        in_specs=[vmem(), vmem(), far, far, near],
        out_specs=(vmem(), vmem(), near),
        scratch_shapes=[
            low(32, 256, 128),
            low(16, 128, 128),
            low(32, 256, 256),
            pltpu.VMEM((32, 16, 256), jnp.int32),
            pltpu.SMEM((40,), jnp.int32),
            full(32, 128, 256),
            low(4, 2, 4, 256, 128),
            low(16, 128, 128),
            full(8, 128),
            low(4, 4, 256, 128),
            low(4, 4, 256, 128),
            low(4, 6, 128, 128),
            low(4, 2, 128, 128),
            low(4, 2, 128, 128),
            full(2, 128, 128),
            low(6, 128, 128),
            low(2, 128, 128),
            low(4, 6, 64, 128),
            low(4, 2, 64, 128),
            low(4, 128, 128),
            low(4, 128, 128),
            full(4, 4, 8, 128),
            full(1, 8, 128),
            full(5, 8, 128),
            pltpu.SemaphoreType.DMA((8,)),
            pltpu.SemaphoreType.DMA((N_COPIES,)),
            pltpu.SemaphoreType.DMA((N_COPIES,)),
        ],
        compiler_params=pltpu.CompilerParams(collective_id=0, has_side_effects=True),
        name="fused",
    )(factor_u[0], factor_v[0], values[0, 0], mask_words[0, 0], tile_cols[0, 0])
    return new_u[None], new_v[None], loss[0, 0]


def solution(mesh):
    return jax.shard_map(
        per_device,
        mesh=mesh,
        in_specs=(
            P("rows", "cols", None),
            P("cols", "rows", None),
            P("rows", "cols", None, None, None),
            P("rows", "cols", None, None, None),
            P("rows", "cols", None),
        ),
        out_specs=(P("rows", "cols", None), P("cols", "rows", None), P()),
        check_vma=False,
    )
```

```python
import jax
import jax.numpy as jnp
from jax import lax
from jax.experimental import pallas as pl
from jax.experimental.pallas import tpu as pltpu
from jax.sharding import PartitionSpec as P

F32 = jnp.float32
BF16 = jnp.bfloat16
STEP = 0.01
RIDGE = 0.1
MESH = pl.DeviceIdType.MESH


def wrap(i, n=4):
    return lax.rem(i + n, n)


class Place:
    def __init__(self):
        c = lax.axis_index("cols")
        r = lax.axis_index("rows")
        self.c, self.r = c, r
        self.k = lax.rem(c, 2)
        self.x = lax.rem(lax.div(c, 2), 4)
        self.zh = lax.div(c, 8)
        self.y = lax.div(r, 4)
        self.zl = lax.rem(r, 4)

    def col(self, dz=0, dx=0, dk=0):
        return wrap(self.zh + dz) * 8 + wrap(self.x + dx) * 2 + lax.rem(self.k + dk, 2)

    def row(self, dy=0, dl=0):
        return wrap(self.y + dy) * 4 + wrap(self.zl + dl)

    def dev(self, dz=0, dx=0, dk=0, dy=0, dl=0):
        if dy or dl:
            return {"rows": self.row(dy, dl)}
        return {"cols": self.col(dz, dx, dk)}


class Net:
    def __init__(self, send_sems, recv_sems):
        self.send_sems, self.recv_sems = send_sems, recv_sems
        self.ids, self.sent = {}, []

    def at(self, name):
        return self.ids.setdefault(name, len(self.ids))

    def send(self, name, src, dst, dev):
        i = self.at(name)
        copy = pltpu.make_async_remote_copy(
            src_ref=src, dst_ref=dst, send_sem=self.send_sems.at[i], recv_sem=self.recv_sems.at[i],
            device_id=dev, device_id_type=MESH)
        copy.start()
        self.sent.append(copy)

    def recv(self, name, ref, dev):
        i = self.at(name)
        pltpu.make_async_remote_copy(
            src_ref=ref, dst_ref=ref, send_sem=self.send_sems.at[i], recv_sem=self.recv_sems.at[i],
            device_id=dev, device_id_type=MESH).wait_recv()

    def finish(self):
        for copy in self.sent:
            copy.wait_send()


DZ = (0, -1, 1, 2)
N_COPIES = 120
UNROLL = 4


def fused_kernel(entries, fu_hbm, fv_hbm, vals_hbm, mask_hbm, ids_ref, nu_ref, nv_ref, loss_ref,
                 fu_ref, fv_ref, u, v, vals, mask, prev, chain, pu, pv, ls, pb, t, xb, w, w0, zb, yb, wl, wl0, lb, le, ln,
                 load_sems, send_sems, recv_sems):
    p = Place()
    net = Net(send_sems, recv_sems)

    def f(ref):
        return ref[...].astype(F32)

    own = [pltpu.make_async_copy(fu_hbm, fu_ref, load_sems.at[8]), pltpu.make_async_copy(fv_hbm, fv_ref, load_sems.at[9])]
    for copy in own:
        copy.start()
    loads = []
    for j in range(4):
        base = wrap(p.zh + DZ[j]) * 8
        for n, (far, near) in enumerate(((mask_hbm, mask), (vals_hbm, vals))):
            copy = pltpu.make_async_copy(far.at[pl.ds(base, 8)], near.at[pl.ds(base, 8)], load_sems.at[2 * j + n])
            copy.start()
            loads.append(copy)

    peers = ([p.dev(dk=1)] + [p.dev(dx=d) for d in (1, 2, 3)] + [p.dev(dz=d) for d in (1, 2, 3)]
             + [p.dev(dy=d) for d in (1, 2, 3)] + [p.dev(dl=d) for d in (1, 2, 3)])
    barrier = pltpu.get_barrier_semaphore()
    for peer in peers:
        pl.semaphore_signal(barrier, inc=1, device_id=peer, device_id_type=MESH)
    for copy in own:
        copy.wait()
    u[p.c] = fu_ref[...].astype(BF16)
    v[p.r] = fv_ref[...].astype(BF16)
    pl.semaphore_wait(barrier, len(peers))


    def ub(j, dx, h):
        return u.at[p.col(DZ[j], dx), pl.ds(h * 128, 128)]

    def xput(j, h):
        for d in (1, -1, 2):
            ref = ub(j, 0, h)
            net.send(("gx", j, d, h), ref, ref, p.dev(dx=d))

    def xin(j, d):
        for h in (0, 1):
            net.recv(("gx", j, d, h), ub(j, -d, h), p.dev(dx=d))
        twin(j, -d)

    def yput(l):
        ref = v.at[p.row(0, l)]
        for d in (1, -1, 2):
            net.send(("gy", l, d), ref, ref, p.dev(dy=d))

    def yin(l):
        for d in (1, -1, 2):
            net.recv(("gy", l, d), v.at[p.row(-d, l)], p.dev(dy=d))

    def twin(j, dx):
        dx %= 4
        ref = u.at[p.col(DZ[j], dx)]
        net.send(("gp", j, dx), ref, ref, p.dev(dk=1))

    def z_in(s, h, j):
        ref = ub(j, 0, h)
        net.recv(("gz", s, h), ref, p.dev(dz=s))
        if (s, h) in ((1, 0), (-1, 1)):
            net.send(("gz", s, "hop"), ref, ref, p.dev(dz=s))
        xput(j, h)

    def z_far():
        for s, h in ((1, 0), (-1, 1)):
            net.recv(("gz", s, "hop"), ub(3, 0, h), p.dev(dz=s))
            xput(3, h)
        twin(3, 0)


    order = (0, 1, 2, 3)
    probe = jnp.left_shift(1, lax.rem(lax.broadcasted_iota(jnp.int32, (16, 256), 0), 16))

    def links():
        last = [jnp.int32(-1)] * 8
        for n in range(32):
            j, i = order[n // 8], (0, 1, 3, 2)[n % 8 // 2]
            q = ids_ref[p.col(DZ[j], i, n % 2)]
            before = jnp.int32(-1)
            for tile in range(8):
                hit = q == tile
                before = jnp.where(hit, last[tile], before)
                last[tile] = jnp.where(hit, n, last[tile])
            prev[n] = before
        for tile in range(8):
            prev[32 + tile] = last[tile]

    def linked(n):
        return jnp.where(n >= 0, chain[jnp.maximum(n, 0)], 0.0)

    def work(j, part, squares):
        for dx in ((0, 1), (3, 2))[part]:
            net.recv(("gp", j, dx), u.at[p.col(DZ[j], dx, 1)], p.dev(dk=1))
        if part == 0:
            loads[2 * j].wait()
            loads[2 * j + 1].wait()
        zj = wrap(p.zh + DZ[j])
        first = order.index(j) * 8 + 4 * part

        def slot(m, squares):
            i = lax.div(m, 2) if part == 0 else 3 - lax.div(m, 2)
            kk = lax.rem(m, 2)
            s = zj * 8 + lax.rem(p.x + i, 4) * 2 + lax.rem(p.k + kk, 2)
            q = ids_ref[s]
            ut = u[s]
            vt = v[pl.ds(2 * q, 2)].reshape(256, 128)
            pred = lax.dot_general(ut, vt, (((1,), (1,)), ((), ())), preferred_element_type=F32)
            bits = jnp.concatenate(
                [jnp.bitwise_and(jnp.broadcast_to(mask[s, b:b + 1, :], (16, 256)), probe) for b in range(16)], axis=0)
            res = jnp.where(bits != 0, pred - vals[s].astype(F32), 0.0)
            low = res.astype(BF16)
            pu[j, kk, i] = jnp.dot(low, vt, preferred_element_type=F32).astype(BF16)
            chain[first + m] = linked(prev[first + m]) + lax.dot_general(
                ut, low, (((0,), (0,)), ((), ())), preferred_element_type=F32)
            return squares + jnp.sum((res * res).reshape(32, 8, 256), axis=0)

        squares = lax.fori_loop(0, 4, slot, squares, unroll=UNROLL)
        rows = pl.ds(2 * part, 2)
        net.send(("p", j, part), pu.at[j, 1, rows], pb.at[j, rows], p.dev(dk=1))
        return squares


    def s1(j):
        for part in (0, 1):
            rows = pl.ds(2 * part, 2)
            net.recv(("p", j, part), pb.at[j, rows], p.dev(dk=1))
        for i in (2, 1, 3):
            t[j, i] = (f(pu.at[j, 0, i]) + f(pb.at[j, i])).astype(BF16)
            net.send(("x", j, i), t.at[j, i], xb.at[j, i], p.dev(dx=i))
        xb[j, 0] = (f(pu.at[j, 0, 0]) + f(pb.at[j, 0])).astype(BF16)

    def s3(j):
        for i in (1, 3, 2):
            net.recv(("x", j, i), xb.at[j, i], p.dev(dx=i))
        total = (f(xb.at[j, 0]) + f(xb.at[j, 1])) + (f(xb.at[j, 2]) + f(xb.at[j, 3]))
        if j == 0:
            w0[...] = total
        else:
            w[j] = total.astype(BF16)
            net.send(("z", j), w.at[j], zb.at[j], p.dev(dz=DZ[j]))

    def yopen(l):
        for i in (2, 1, 3):
            net.send(("y", l, i), pv.at[p.row(i, l)], yb.at[l, i], p.dev(dy=i))

    def yclose(l):
        for i in (1, 3, 2):
            net.recv(("y", l, i), yb.at[l, i], p.dev(dy=i))
        total = (f(pv.at[p.row(0, l)]) + f(yb.at[l, 1])) + (f(yb.at[l, 2]) + f(yb.at[l, 3]))
        if l:
            wl[l] = total.astype(BF16)
            net.send(("l", l), wl.at[l], wl0.at[l], p.dev(dl=l))
        return total

    def share(n, dev_of):
        for d in (1, 2, 3):
            net.send(("lo", n, d), ln.at[n], lb.at[n, d], dev_of(d))

    def shared(n, dev_of):
        for d in (1, 2, 3):
            net.recv(("lo", n, d), lb.at[n, d], dev_of(d))
        ln[n + 1] = (ln[n] + lb[n, 2]) + (lb[n, 1] + lb[n, 3])

    axes = (lambda d: p.dev(dz=d), lambda d: p.dev(dx=d), lambda d: p.dev(dy=d), lambda d: p.dev(dl=d))


    for d in (1, 2, 3):
        ref = v.at[p.r]
        net.send(("gl", d), ref, ref, p.dev(dl=d))
    yput(0)
    for s, h in ((1, 0), (-1, 1), (1, 1), (-1, 0)):
        ref = ub(0, 0, h)
        net.send(("gz", s, h), ref, ref, p.dev(dz=s))
    for h in (0, 1):
        xput(0, h)
    twin(0, 0)
    fu = fu_ref[...]
    fv = fv_ref[...]
    ridge = (0.5 * RIDGE) * (
        jnp.sum((fu * fu).reshape(32, 8, 128), axis=0) + jnp.sum((fv * fv).reshape(16, 8, 128), axis=0))
    links()
    for d in (1, 3, 2):
        net.recv(("gl", d), v.at[p.row(0, -d)], p.dev(dl=d))
        yput(-d)
    for d in (1, -1, 2):
        xin(0, d)
    z_in(1, 0, 1)
    z_in(-1, 1, 2)
    z_in(1, 1, 1)
    z_in(-1, 0, 2)
    twin(1, 0)
    twin(2, 0)
    for d in (0, 1, 2, 3):
        yin(-d)
    squares = jnp.zeros((8, 256), F32)
    squares = work(0, 0, squares)
    squares = work(0, 1, squares)
    for d in (-1, 1, 2):
        xin(1, d)
    z_far()
    squares = work(1, 0, squares)
    for d in (-1, 1, 2):
        xin(2, d)
    squares = work(1, 1, squares)
    squares = work(2, 0, squares)
    s1(1)
    squares = work(2, 1, squares)
    xin(3, -1)
    xin(3, 1)
    s1(2)
    squares = work(3, 0, squares)
    xin(3, 2)
    s3(1)
    squares = work(3, 1, squares)
    ls[...] = 0.5 * (squares[:, :128] + squares[:, 128:]) + ridge
    net.send(("lp",), ls, le.at[0], p.dev(dk=1))
    for q in range(8):
        pv[pl.ds(2 * q, 2)] = linked(prev[32 + q]).T.astype(BF16).reshape(2, 128, 128)
    for l in (1, 2, 3, 0):
        yopen(l)
    s1(3)
    net.recv(("lp",), le.at[0], p.dev(dk=1))
    ln[0] = ls[...] + le[0]
    share(0, axes[0])
    s1(0)
    s3(2)
    s3(3)
    for l in (1, 2, 3):
        yclose(l)
    mine = yclose(0)
    shared(0, axes[0])
    share(1, axes[1])
    s3(0)
    shared(1, axes[1])
    share(2, axes[2])
    shared(2, axes[2])
    share(3, axes[3])
    for l in (1, 2, 3):
        net.recv(("l", l), wl0.at[l], p.dev(dl=l))
    grad = (mine + f(wl0.at[1])) + (f(wl0.at[2]) + f(wl0.at[3]))
    old = fv_ref[...]
    nv_ref[...] = old - STEP * (grad + RIDGE * old)
    for j in (1, 2, 3):
        net.recv(("z", j), zb.at[j], p.dev(dz=DZ[j]))
    grad = (w0[...] + f(zb.at[1])) + (f(zb.at[2]) + f(zb.at[3]))
    old = fu_ref[...]
    nu_ref[...] = old - STEP * (grad + RIDGE * old)
    shared(3, axes[3])
    loss_ref[0, 0] = jnp.sum(ln[4]) * (1.0 / entries)
    net.finish()


def vmem():
    return pl.BlockSpec(memory_space=pltpu.VMEM)


def per_device(factor_u, factor_v, values, mask_words, tile_cols):
    entries = lax.axis_size("rows") * lax.axis_size("cols") * 32 * 256 * 256
    far = pl.BlockSpec(memory_space=pltpu.HBM)
    near = pl.BlockSpec(memory_space=pltpu.SMEM)

    def low(*shape):
        return pltpu.VMEM(shape, BF16)

    def full(*shape):
        return pltpu.VMEM(shape, F32)

    new_u, new_v, loss = pl.pallas_call(
        lambda *refs: fused_kernel(entries, *refs),
        out_shape=(jax.ShapeDtypeStruct((256, 128), F32), jax.ShapeDtypeStruct((128, 128), F32),
                   jax.ShapeDtypeStruct((1, 1), F32)),
        in_specs=[far, far, far, far, near],
        out_specs=(vmem(), vmem(), near),
        scratch_shapes=[
            full(256, 128),
            full(128, 128),
            low(32, 256, 128),
            low(16, 128, 128),
            low(32, 256, 256),
            pltpu.VMEM((32, 16, 256), jnp.int32),
            pltpu.SMEM((40,), jnp.int32),
            full(32, 128, 256),
            low(4, 2, 4, 256, 128),
            low(16, 128, 128),
            full(8, 128),
            low(4, 4, 256, 128),
            low(4, 4, 256, 128),
            low(4, 4, 256, 128),
            low(4, 256, 128),
            full(256, 128),
            low(4, 256, 128),
            low(4, 4, 128, 128),
            low(4, 128, 128),
            low(4, 128, 128),
            full(4, 4, 8, 128),
            full(1, 8, 128),
            full(5, 8, 128),
            pltpu.SemaphoreType.DMA((10,)),
            pltpu.SemaphoreType.DMA((N_COPIES,)),
            pltpu.SemaphoreType.DMA((N_COPIES,)),
        ],
        compiler_params=pltpu.CompilerParams(collective_id=0, has_side_effects=True),
        name="fused",
    )(factor_u[0], factor_v[0], values[0, 0], mask_words[0, 0], tile_cols[0, 0])
    return new_u[None], new_v[None], loss[0, 0]


def solution(mesh):
    return jax.shard_map(
        per_device,
        mesh=mesh,
        in_specs=(
            P("rows", "cols", None),
            P("cols", "rows", None),
            P("rows", "cols", None, None, None),
            P("rows", "cols", None, None, None),
            P("rows", "cols", None),
        ),
        out_specs=(P("rows", "cols", None), P("cols", "rows", None), P()),
        check_vma=False,
    )
```

```python
import jax
import jax.numpy as jnp
from jax import lax
from jax.experimental import pallas as pl
from jax.experimental.pallas import tpu as pltpu
from jax.sharding import PartitionSpec as P

F32 = jnp.float32
BF16 = jnp.bfloat16
STEP = 0.01
RIDGE = 0.1
MESH = pl.DeviceIdType.MESH


def wrap(i, n=4):
    return lax.rem(i + n, n)


class Place:
    def __init__(self):
        c = lax.axis_index("cols")
        r = lax.axis_index("rows")
        self.c, self.r = c, r
        self.k = lax.rem(c, 2)
        self.x = lax.rem(lax.div(c, 2), 4)
        self.zh = lax.div(c, 8)
        self.y = lax.div(r, 4)
        self.zl = lax.rem(r, 4)

    def col(self, dz=0, dx=0, dk=0):
        return wrap(self.zh + dz) * 8 + wrap(self.x + dx) * 2 + lax.rem(self.k + dk, 2)

    def row(self, dy=0, dl=0):
        return wrap(self.y + dy) * 4 + wrap(self.zl + dl)

    def dev(self, dz=0, dx=0, dk=0, dy=0, dl=0):
        if dy or dl:
            return {"rows": self.row(dy, dl)}
        return {"cols": self.col(dz, dx, dk)}


class Net:
    def __init__(self, send_sems, recv_sems):
        self.send_sems, self.recv_sems = send_sems, recv_sems
        self.ids, self.sent = {}, []

    def at(self, name):
        return self.ids.setdefault(name, len(self.ids))

    def send(self, name, src, dst, dev):
        i = self.at(name)
        copy = pltpu.make_async_remote_copy(
            src_ref=src, dst_ref=dst, send_sem=self.send_sems.at[i], recv_sem=self.recv_sems.at[i],
            device_id=dev, device_id_type=MESH)
        copy.start()
        self.sent.append(copy)

    def recv(self, name, ref, dev):
        i = self.at(name)
        pltpu.make_async_remote_copy(
            src_ref=ref, dst_ref=ref, send_sem=self.send_sems.at[i], recv_sem=self.recv_sems.at[i],
            device_id=dev, device_id_type=MESH).wait_recv()

    def finish(self):
        for copy in self.sent:
            copy.wait_send()


DZ = (0, -1, 1, 2)
N_COPIES = 140
UNROLL = 4


def fused_kernel(entries, fu_hbm, fv_hbm, vals_hbm, mask_hbm, ids_ref, nu_ref, nv_ref, loss_ref,
                 fu_ref, fv_ref, u, v, vals, mask, prev, chain, pu, pv, ls, pb, t, xb, w, w0, zb, yb, wl, wl0, lb, le, ln, lz, lx,
                 load_sems, send_sems, recv_sems):
    p = Place()
    net = Net(send_sems, recv_sems)

    def f(ref):
        return ref[...].astype(F32)

    own = [pltpu.make_async_copy(fu_hbm, fu_ref, load_sems.at[8]), pltpu.make_async_copy(fv_hbm, fv_ref, load_sems.at[9])]
    for copy in own:
        copy.start()
    loads = []
    for j in range(4):
        base = wrap(p.zh + DZ[j]) * 8
        for n, (far, near) in enumerate(((mask_hbm, mask), (vals_hbm, vals))):
            copy = pltpu.make_async_copy(far.at[pl.ds(base, 8)], near.at[pl.ds(base, 8)], load_sems.at[2 * j + n])
            copy.start()
            loads.append(copy)

    def zdev(d):
        place = lax.rem(p.zh * 4 + p.zl + d, 16)
        return {"cols": lax.div(place, 4) * 8 + p.x * 2 + p.k, "rows": p.y * 4 + lax.rem(place, 4)}

    peers = ([p.dev(dk=1)] + [p.dev(dx=d) for d in (1, 2, 3)] + [p.dev(dy=d) for d in (1, 2, 3)]
             + [zdev(d) for d in range(1, 16)])
    barrier = pltpu.get_barrier_semaphore()
    for peer in peers:
        pl.semaphore_signal(barrier, inc=1, device_id=peer, device_id_type=MESH)
    for copy in own:
        copy.wait()
    u[p.c] = fu_ref[...].astype(BF16)
    v[p.r] = fv_ref[...].astype(BF16)
    pl.semaphore_wait(barrier, len(peers))


    def ub(j, dx, h):
        return u.at[p.col(DZ[j], dx), pl.ds(h * 128, 128)]

    def xput(j, h):
        for d in (1, -1, 2):
            ref = ub(j, 0, h)
            net.send(("gx", j, d, h), ref, ref, p.dev(dx=d))

    def xin(j, d):
        for h in (0, 1):
            net.recv(("gx", j, d, h), ub(j, -d, h), p.dev(dx=d))
        twin(j, -d)

    def yput(l):
        ref = v.at[p.row(0, l)]
        for d in (1, -1, 2):
            net.send(("gy", l, d), ref, ref, p.dev(dy=d))

    def yin(l):
        for d in (1, -1, 2):
            net.recv(("gy", l, d), v.at[p.row(-d, l)], p.dev(dy=d))

    def twin(j, dx):
        dx %= 4
        ref = u.at[p.col(DZ[j], dx)]
        net.send(("gp", j, dx), ref, ref, p.dev(dk=1))

    def z_in(s, h, j):
        ref = ub(j, 0, h)
        net.recv(("gz", s, h), ref, p.dev(dz=s))
        if (s, h) in ((1, 0), (-1, 1)):
            net.send(("gz", s, "hop"), ref, ref, p.dev(dz=s))
        xput(j, h)

    def z_far():
        for s, h in ((1, 0), (-1, 1)):
            net.recv(("gz", s, "hop"), ub(3, 0, h), p.dev(dz=s))
            xput(3, h)
        twin(3, 0)


    order = (0, 1, 2, 3)
    probe = jnp.left_shift(1, lax.rem(lax.broadcasted_iota(jnp.int32, (16, 256), 0), 16))

    def links():
        last = [jnp.int32(-1)] * 8
        for n in range(32):
            j, i = order[n // 8], (0, 1, 3, 2)[n % 8 // 2]
            q = ids_ref[p.col(DZ[j], i, n % 2)]
            before = jnp.int32(-1)
            for tile in range(8):
                hit = q == tile
                before = jnp.where(hit, last[tile], before)
                last[tile] = jnp.where(hit, n, last[tile])
            prev[n] = before
        for tile in range(8):
            prev[32 + tile] = last[tile]

    def linked(n):
        return jnp.where(n >= 0, chain[jnp.maximum(n, 0)], 0.0)

    def work(j, part, squares):
        for dx in ((0, 1), (3, 2))[part]:
            net.recv(("gp", j, dx), u.at[p.col(DZ[j], dx, 1)], p.dev(dk=1))
        if part == 0:
            loads[2 * j].wait()
            loads[2 * j + 1].wait()
        zj = wrap(p.zh + DZ[j])
        first = order.index(j) * 8 + 4 * part

        def slot(m, squares):
            i = lax.div(m, 2) if part == 0 else 3 - lax.div(m, 2)
            kk = lax.rem(m, 2)
            s = zj * 8 + lax.rem(p.x + i, 4) * 2 + lax.rem(p.k + kk, 2)
            q = ids_ref[s]
            ut = u[s]
            vt = v[pl.ds(2 * q, 2)].reshape(256, 128)
            pred = lax.dot_general(ut, vt, (((1,), (1,)), ((), ())), preferred_element_type=F32)
            bits = jnp.concatenate(
                [jnp.bitwise_and(jnp.broadcast_to(mask[s, b:b + 1, :], (16, 256)), probe) for b in range(16)], axis=0)
            res = jnp.where(bits != 0, pred - vals[s].astype(F32), 0.0)
            low = res.astype(BF16)
            pu[j, kk, i] = jnp.dot(low, vt, preferred_element_type=F32).astype(BF16)
            chain[first + m] = linked(prev[first + m]) + lax.dot_general(
                ut, low, (((0,), (0,)), ((), ())), preferred_element_type=F32)
            return squares + jnp.sum((res * res).reshape(32, 8, 256), axis=0)

        squares = lax.fori_loop(0, 4, slot, squares, unroll=UNROLL)
        rows = pl.ds(2 * part, 2)
        net.send(("p", j, part), pu.at[j, 1, rows], pb.at[j, rows], p.dev(dk=1))
        return squares


    halves = {0: (slice(0, 256),), 1: (slice(0, 256),), 2: (slice(0, 256),), 3: (slice(0, 128), slice(128, 256))}

    def cut(j, h):
        return pl.ds(halves[j][h].start, halves[j][h].stop - halves[j][h].start)

    def s1(j, part):
        rows = pl.ds(2 * part, 2)
        net.recv(("p", j, part), pb.at[j, rows], p.dev(dk=1))
        for h in range(len(halves[j])):
            r = cut(j, h)
            for i in ((1,), (2, 3))[part]:
                t[j, i, r] = (f(pu.at[j, 0, i, r]) + f(pb.at[j, i, r])).astype(BF16)
                net.send(("x", j, i, h), t.at[j, i, r], xb.at[j, i, r], p.dev(dx=i))
        if part == 0:
            xb[j, 0] = (f(pu.at[j, 0, 0]) + f(pb.at[j, 0])).astype(BF16)

    def s3(j):
        for h in range(len(halves[j])):
            r = cut(j, h)
            for i in (1, 3, 2):
                net.recv(("x", j, i, h), xb.at[j, i, r], p.dev(dx=i))
            total = (f(xb.at[j, 0, r]) + f(xb.at[j, 1, r])) + (f(xb.at[j, 2, r]) + f(xb.at[j, 3, r]))
            if j == 0:
                w0[...] = total
            else:
                w[j, r] = total.astype(BF16)
                net.send(("z", j, h), w.at[j, r], zb.at[j, r], p.dev(dz=DZ[j]))

    def yopen(l):
        for i in (2, 1, 3):
            net.send(("y", l, i), pv.at[p.row(i, l)], yb.at[l, i], p.dev(dy=i))

    def yclose(l):
        for i in (1, 3, 2):
            net.recv(("y", l, i), yb.at[l, i], p.dev(dy=i))
        total = (f(pv.at[p.row(0, l)]) + f(yb.at[l, 1])) + (f(yb.at[l, 2]) + f(yb.at[l, 3]))
        if l:
            wl[l] = total.astype(BF16)
            net.send(("l", l), wl.at[l], wl0.at[l], p.dev(dl=l))
        return total

    def share(n, dev_of):
        for d in (1, 2, 3):
            net.send(("lo", n, d), ln.at[n], lb.at[n, d], dev_of(d))

    def shared(n, dev_of):
        for d in (1, 2, 3):
            net.recv(("lo", n, d), lb.at[n, d], dev_of(d))
        ln[n + 1] = (ln[n] + lb[n, 2]) + (lb[n, 1] + lb[n, 3])

    axes = (lambda d: p.dev(dx=d), lambda d: p.dev(dy=d))


    def zput(s, h):
        ref = ub(0, 0, h)
        net.send(("gz", s, h), ref, ref, p.dev(dz=s))

    zput(1, 0)
    zput(-1, 1)
    for d in (1, 2, 3):
        ref = v.at[p.r]
        net.send(("gl", d), ref, ref, p.dev(dl=d))
    zput(1, 1)
    zput(-1, 0)
    yput(0)
    for h in (0, 1):
        xput(0, h)
    twin(0, 0)
    fu = fu_ref[...]
    fv = fv_ref[...]
    ridge = (0.5 * RIDGE) * (
        jnp.sum((fu * fu).reshape(32, 8, 128), axis=0) + jnp.sum((fv * fv).reshape(16, 8, 128), axis=0))
    links()
    for d in (1, 3, 2):
        net.recv(("gl", d), v.at[p.row(0, -d)], p.dev(dl=d))
        yput(-d)
    for d in (1, -1, 2):
        xin(0, d)
    z_in(1, 0, 1)
    z_in(-1, 1, 2)
    z_in(1, 1, 1)
    z_in(-1, 0, 2)
    twin(1, 0)
    twin(2, 0)
    for d in (0, 1, 2, 3):
        yin(-d)
    squares = jnp.zeros((8, 256), F32)
    squares = work(0, 0, squares)
    for d in (-1, 1):
        xin(1, d)
    squares = work(0, 1, squares)
    xin(1, 2)
    z_far()
    squares = work(1, 0, squares)
    for d in (-1, 1, 2):
        xin(2, d)
    squares = work(1, 1, squares)
    squares = work(2, 0, squares)
    s1(1, 0)
    s1(1, 1)
    xin(3, -1)
    xin(3, 1)
    squares = work(2, 1, squares)
    s1(2, 0)
    xin(3, 2)
    squares = work(3, 0, squares)
    s1(2, 1)
    squares = work(3, 1, squares)
    ls[...] = jnp.sum(0.5 * (squares[:, :128] + squares[:, 128:]) + ridge, axis=0, keepdims=True)
    net.send(("lp",), ls, le.at[0], p.dev(dk=1))
    s1(3, 0)
    for q in range(8):
        pv[pl.ds(2 * q, 2)] = linked(prev[32 + q]).T.astype(BF16).reshape(2, 128, 128)
    for l in (1, 2, 3, 0):
        yopen(l)
    s1(3, 1)
    net.recv(("lp",), le.at[0], p.dev(dk=1))
    total = ls[...] + le[0]
    here = p.zh * 4 + p.zl
    lz[here] = total
    lx[0] = total
    for d in range(1, 16):
        net.send(("lz", d), lx.at[0], lz.at[here], zdev(d))
    s3(1)
    s3(2)
    s1(0, 0)
    s1(0, 1)
    s3(3)
    for l in (1, 2, 3):
        yclose(l)
    mine = yclose(0)
    for d in range(1, 16):
        net.recv(("lz", d), lz.at[lax.rem(here + 16 - d, 16)], zdev(d))
    ln[0] = jnp.sum(lz[...], axis=0)
    share(0, axes[0])
    s3(0)
    shared(0, axes[0])
    share(1, axes[1])
    for l in (1, 2, 3):
        net.recv(("l", l), wl0.at[l], p.dev(dl=l))
    grad = (mine + f(wl0.at[1])) + (f(wl0.at[2]) + f(wl0.at[3]))
    old = fv_ref[...]
    nv_ref[...] = old - STEP * (grad + RIDGE * old)
    shared(1, axes[1])
    loss_ref[0, 0] = jnp.sum(ln[2]) * (1.0 / entries)
    for j in (1, 2, 3):
        for h in range(len(halves[j])):
            net.recv(("z", j, h), zb.at[j, cut(j, h)], p.dev(dz=DZ[j]))
    grad = (w0[...] + f(zb.at[1])) + (f(zb.at[2]) + f(zb.at[3]))
    old = fu_ref[...]
    nu_ref[...] = old - STEP * (grad + RIDGE * old)
    net.finish()


def vmem():
    return pl.BlockSpec(memory_space=pltpu.VMEM)


def per_device(factor_u, factor_v, values, mask_words, tile_cols):
    entries = lax.axis_size("rows") * lax.axis_size("cols") * 32 * 256 * 256
    far = pl.BlockSpec(memory_space=pltpu.HBM)
    near = pl.BlockSpec(memory_space=pltpu.SMEM)

    def low(*shape):
        return pltpu.VMEM(shape, BF16)

    def full(*shape):
        return pltpu.VMEM(shape, F32)

    new_u, new_v, loss = pl.pallas_call(
        lambda *refs: fused_kernel(entries, *refs),
        out_shape=(jax.ShapeDtypeStruct((256, 128), F32), jax.ShapeDtypeStruct((128, 128), F32),
                   jax.ShapeDtypeStruct((1, 1), F32)),
        in_specs=[far, far, far, far, near],
        out_specs=(vmem(), vmem(), near),
        scratch_shapes=[
            full(256, 128),
            full(128, 128),
            low(32, 256, 128),
            low(16, 128, 128),
            low(32, 256, 256),
            pltpu.VMEM((32, 16, 256), jnp.int32),
            pltpu.SMEM((40,), jnp.int32),
            full(32, 128, 256),
            low(4, 2, 4, 256, 128),
            low(16, 128, 128),
            full(1, 128),
            low(4, 4, 256, 128),
            low(4, 4, 256, 128),
            low(4, 4, 256, 128),
            low(4, 256, 128),
            full(256, 128),
            low(4, 256, 128),
            low(4, 4, 128, 128),
            low(4, 128, 128),
            low(4, 128, 128),
            full(4, 4, 1, 128),
            full(1, 1, 128),
            full(5, 1, 128),
            full(16, 1, 128),
            full(1, 1, 128),
            pltpu.SemaphoreType.DMA((10,)),
            pltpu.SemaphoreType.DMA((N_COPIES,)),
            pltpu.SemaphoreType.DMA((N_COPIES,)),
        ],
        compiler_params=pltpu.CompilerParams(collective_id=0, has_side_effects=True),
        name="fused",
    )(factor_u[0], factor_v[0], values[0, 0], mask_words[0, 0], tile_cols[0, 0])
    return new_u[None], new_v[None], loss[0, 0]


def solution(mesh):
    return jax.shard_map(
        per_device,
        mesh=mesh,
        in_specs=(
            P("rows", "cols", None),
            P("cols", "rows", None),
            P("rows", "cols", None, None, None),
            P("rows", "cols", None, None, None),
            P("rows", "cols", None),
        ),
        out_specs=(P("rows", "cols", None), P("cols", "rows", None), P()),
        check_vma=False,
    )
```

```python
import jax
import jax.numpy as jnp
from jax import lax
from jax.experimental import pallas as pl
from jax.experimental.pallas import tpu as pltpu
from jax.sharding import PartitionSpec as P

F32 = jnp.float32
BF16 = jnp.bfloat16
STEP = 0.01
RIDGE = 0.1
MESH = pl.DeviceIdType.MESH


def wrap(i, n=4):
    return lax.rem(i + n, n)


class Place:
    def __init__(self):
        c = lax.axis_index("cols")
        r = lax.axis_index("rows")
        self.c, self.r = c, r
        self.k = lax.rem(c, 2)
        self.x = lax.rem(lax.div(c, 2), 4)
        self.zh = lax.div(c, 8)
        self.y = lax.div(r, 4)
        self.zl = lax.rem(r, 4)

    def col(self, dz=0, dx=0, dk=0):
        return wrap(self.zh + dz) * 8 + wrap(self.x + dx) * 2 + lax.rem(self.k + dk, 2)

    def row(self, dy=0, dl=0):
        return wrap(self.y + dy) * 4 + wrap(self.zl + dl)

    def dev(self, dz=0, dx=0, dk=0, dy=0, dl=0):
        if dy or dl:
            return {"rows": self.row(dy, dl)}
        return {"cols": self.col(dz, dx, dk)}


class Net:
    def __init__(self, send_sems, recv_sems):
        self.send_sems, self.recv_sems = send_sems, recv_sems
        self.ids, self.sent = {}, []

    def at(self, name):
        return self.ids.setdefault(name, len(self.ids))

    def send(self, name, src, dst, dev):
        i = self.at(name)
        copy = pltpu.make_async_remote_copy(
            src_ref=src, dst_ref=dst, send_sem=self.send_sems.at[i], recv_sem=self.recv_sems.at[i],
            device_id=dev, device_id_type=MESH)
        copy.start()
        self.sent.append(copy)

    def recv(self, name, ref, dev):
        i = self.at(name)
        pltpu.make_async_remote_copy(
            src_ref=ref, dst_ref=ref, send_sem=self.send_sems.at[i], recv_sem=self.recv_sems.at[i],
            device_id=dev, device_id_type=MESH).wait_recv()

    def finish(self):
        for copy in self.sent:
            copy.wait_send()


DZ = (0, -1, 1, 2)
N_COPIES = 140
UNROLL = 4


def fused_kernel(entries, fu_hbm, fv_hbm, vals_hbm, mask_hbm, ids_ref, out_ref, loss_ref,
                 fu_ref, fv_ref, u, v, vals, mask, prev, chain, pu, pv, ls, pb, t, xb, w, w0, zb, yb, wl, wl0, lb, le, ln, lz, lx,
                 load_sems, send_sems, recv_sems):
    p = Place()
    net = Net(send_sems, recv_sems)

    def f(ref):
        return ref[...].astype(F32)

    own = [pltpu.make_async_copy(fu_hbm, fu_ref, load_sems.at[8]), pltpu.make_async_copy(fv_hbm, fv_ref, load_sems.at[9])]
    for copy in own:
        copy.start()
    loads = []
    for j in range(4):
        base = wrap(p.zh + DZ[j]) * 8
        for n, (far, near) in enumerate(((mask_hbm, mask), (vals_hbm, vals))):
            copy = pltpu.make_async_copy(far.at[pl.ds(base, 8)], near.at[pl.ds(base, 8)], load_sems.at[2 * j + n])
            copy.start()
            loads.append(copy)

    def zdev(d):
        place = lax.rem(p.zh * 4 + p.zl + d, 16)
        return {"cols": lax.div(place, 4) * 8 + p.x * 2 + p.k, "rows": p.y * 4 + lax.rem(place, 4)}

    peers = ([p.dev(dk=1)] + [p.dev(dx=d) for d in (1, 2, 3)] + [p.dev(dy=d) for d in (1, 2, 3)]
             + [zdev(d) for d in range(1, 16)])
    barrier = pltpu.get_barrier_semaphore()
    for peer in peers:
        pl.semaphore_signal(barrier, inc=1, device_id=peer, device_id_type=MESH)
    for copy in own:
        copy.wait()
    u[p.c] = fu_ref[...].astype(BF16)
    v[p.r] = fv_ref[...].astype(BF16)
    pl.semaphore_wait(barrier, len(peers))


    def ub(j, dx, h):
        return u.at[p.col(DZ[j], dx), pl.ds(h * 128, 128)]

    def xput(j, h):
        for d in (1, -1, 2):
            ref = ub(j, 0, h)
            net.send(("gx", j, d, h), ref, ref, p.dev(dx=d))

    def xin(j, d):
        for h in (0, 1):
            net.recv(("gx", j, d, h), ub(j, -d, h), p.dev(dx=d))
        twin(j, -d)

    def yput(l):
        ref = v.at[p.row(0, l)]
        for d in (1, -1, 2):
            net.send(("gy", l, d), ref, ref, p.dev(dy=d))

    def yin(l):
        for d in (1, -1, 2):
            net.recv(("gy", l, d), v.at[p.row(-d, l)], p.dev(dy=d))

    def twin(j, dx):
        dx %= 4
        ref = u.at[p.col(DZ[j], dx)]
        net.send(("gp", j, dx), ref, ref, p.dev(dk=1))

    def z_in(s, h, j):
        ref = ub(j, 0, h)
        net.recv(("gz", s, h), ref, p.dev(dz=s))
        if (s, h) in ((1, 0), (-1, 1)):
            net.send(("gz", s, "hop"), ref, ref, p.dev(dz=s))
        xput(j, h)

    def z_far():
        for s, h in ((1, 0), (-1, 1)):
            net.recv(("gz", s, "hop"), ub(3, 0, h), p.dev(dz=s))
            xput(3, h)
        twin(3, 0)


    order = (0, 1, 2, 3)
    probe = jnp.left_shift(1, lax.rem(lax.broadcasted_iota(jnp.int32, (16, 256), 0), 16))

    def links():
        last = [jnp.int32(-1)] * 8
        for n in range(32):
            j, i = order[n // 8], (0, 1, 3, 2)[n % 8 // 2]
            q = ids_ref[p.col(DZ[j], i, n % 2)]
            before = jnp.int32(-1)
            for tile in range(8):
                hit = q == tile
                before = jnp.where(hit, last[tile], before)
                last[tile] = jnp.where(hit, n, last[tile])
            prev[n] = before
        for tile in range(8):
            prev[32 + tile] = last[tile]

    def linked(n):
        return jnp.where(n >= 0, chain[jnp.maximum(n, 0)], 0.0)

    def work(j, part, squares):
        for dx in ((0, 1), (3, 2))[part]:
            net.recv(("gp", j, dx), u.at[p.col(DZ[j], dx, 1)], p.dev(dk=1))
        if part == 0:
            loads[2 * j].wait()
            loads[2 * j + 1].wait()
        zj = wrap(p.zh + DZ[j])
        first = order.index(j) * 8 + 4 * part

        def slot(m, squares):
            i = lax.div(m, 2) if part == 0 else 3 - lax.div(m, 2)
            kk = lax.rem(m, 2)
            s = zj * 8 + lax.rem(p.x + i, 4) * 2 + lax.rem(p.k + kk, 2)
            q = ids_ref[s]
            ut = u[s]
            vt = v[pl.ds(2 * q, 2)].reshape(256, 128)
            pred = lax.dot_general(ut, vt, (((1,), (1,)), ((), ())), preferred_element_type=F32)
            bits = jnp.concatenate(
                [jnp.bitwise_and(jnp.broadcast_to(mask[s, b:b + 1, :], (16, 256)), probe) for b in range(16)], axis=0)
            res = jnp.where(bits != 0, pred - vals[s].astype(F32), 0.0)
            low = res.astype(BF16)
            pu[j, kk, i] = jnp.dot(low, vt, preferred_element_type=F32).astype(BF16)
            chain[first + m] = linked(prev[first + m]) + lax.dot_general(
                ut, low, (((0,), (0,)), ((), ())), preferred_element_type=F32)
            return squares + jnp.sum((res * res).reshape(32, 8, 256), axis=0)

        squares = lax.fori_loop(0, 4, slot, squares, unroll=UNROLL)
        rows = pl.ds(2 * part, 2)
        net.send(("p", j, part), pu.at[j, 1, rows], pb.at[j, rows], p.dev(dk=1))
        return squares


    halves = {0: (slice(0, 256),), 1: (slice(0, 256),), 2: (slice(0, 256),), 3: (slice(0, 128), slice(128, 256))}

    def cut(j, h):
        return pl.ds(halves[j][h].start, halves[j][h].stop - halves[j][h].start)

    def s1(j, part):
        rows = pl.ds(2 * part, 2)
        net.recv(("p", j, part), pb.at[j, rows], p.dev(dk=1))
        for h in range(len(halves[j])):
            r = cut(j, h)
            for i in ((1,), (2, 3))[part]:
                t[j, i, r] = (f(pu.at[j, 0, i, r]) + f(pb.at[j, i, r])).astype(BF16)
                net.send(("x", j, i, h), t.at[j, i, r], xb.at[j, i, r], p.dev(dx=i))
        if part == 0:
            xb[j, 0] = (f(pu.at[j, 0, 0]) + f(pb.at[j, 0])).astype(BF16)

    def s3(j):
        for h in range(len(halves[j])):
            r = cut(j, h)
            for i in (1, 3, 2):
                net.recv(("x", j, i, h), xb.at[j, i, r], p.dev(dx=i))
            total = (f(xb.at[j, 0, r]) + f(xb.at[j, 1, r])) + (f(xb.at[j, 2, r]) + f(xb.at[j, 3, r]))
            if j == 0:
                w0[...] = total
            else:
                w[j, r] = total.astype(BF16)
                net.send(("z", j, h), w.at[j, r], zb.at[j, r], p.dev(dz=DZ[j]))

    def yopen(l):
        for i in (2, 1, 3):
            net.send(("y", l, i), pv.at[p.row(i, l)], yb.at[l, i], p.dev(dy=i))

    def yclose(l):
        for i in (1, 3, 2):
            net.recv(("y", l, i), yb.at[l, i], p.dev(dy=i))
        total = (f(pv.at[p.row(0, l)]) + f(yb.at[l, 1])) + (f(yb.at[l, 2]) + f(yb.at[l, 3]))
        if l:
            wl[l] = total.astype(BF16)
            net.send(("l", l), wl.at[l], wl0.at[l], p.dev(dl=l))
        return total

    def share(n, dev_of):
        for d in (1, 2, 3):
            net.send(("lo", n, d), ln.at[n], lb.at[n, d], dev_of(d))

    def shared(n, dev_of):
        for d in (1, 2, 3):
            net.recv(("lo", n, d), lb.at[n, d], dev_of(d))
        ln[n + 1] = (ln[n] + lb[n, 2]) + (lb[n, 1] + lb[n, 3])

    axes = (lambda d: p.dev(dx=d), lambda d: p.dev(dy=d))


    def zput(s, h):
        ref = ub(0, 0, h)
        net.send(("gz", s, h), ref, ref, p.dev(dz=s))

    zput(1, 0)
    zput(-1, 1)
    for d in (1, 2, 3):
        ref = v.at[p.r]
        net.send(("gl", d), ref, ref, p.dev(dl=d))
    zput(1, 1)
    zput(-1, 0)
    yput(0)
    for h in (0, 1):
        xput(0, h)
    twin(0, 0)
    fu = fu_ref[...]
    fv = fv_ref[...]
    ridge = (0.5 * RIDGE) * (
        jnp.sum((fu * fu).reshape(32, 8, 128), axis=0) + jnp.sum((fv * fv).reshape(16, 8, 128), axis=0))
    links()
    for d in (1, 3, 2):
        net.recv(("gl", d), v.at[p.row(0, -d)], p.dev(dl=d))
        yput(-d)
    for d in (1, -1, 2):
        xin(0, d)
    z_in(1, 0, 1)
    z_in(-1, 1, 2)
    z_in(1, 1, 1)
    z_in(-1, 0, 2)
    twin(1, 0)
    twin(2, 0)
    for d in (0, 1, 2, 3):
        yin(-d)
    squares = jnp.zeros((8, 256), F32)
    squares = work(0, 0, squares)
    for d in (-1, 1):
        xin(1, d)
    squares = work(0, 1, squares)
    xin(1, 2)
    z_far()
    squares = work(1, 0, squares)
    for d in (-1, 1, 2):
        xin(2, d)
    squares = work(1, 1, squares)
    s1(1, 0)
    squares = work(2, 0, squares)
    s1(1, 1)
    xin(3, -1)
    xin(3, 1)
    squares = work(2, 1, squares)
    s1(2, 0)
    xin(3, 2)
    squares = work(3, 0, squares)
    s1(2, 1)
    squares = work(3, 1, squares)
    ls[...] = jnp.sum(0.5 * (squares[:, :128] + squares[:, 128:]) + ridge, axis=0, keepdims=True)
    net.send(("lp",), ls, le.at[0], p.dev(dk=1))
    s1(3, 0)
    for q in range(8):
        pv[pl.ds(2 * q, 2)] = linked(prev[32 + q]).T.astype(BF16).reshape(2, 128, 128)
    for l in (1, 2, 3, 0):
        yopen(l)
    s1(3, 1)
    net.recv(("lp",), le.at[0], p.dev(dk=1))
    total = ls[...] + le[0]
    here = p.zh * 4 + p.zl
    lz[here] = total
    lx[0] = total
    for d in range(1, 16):
        net.send(("lz", d), lx.at[0], lz.at[here], zdev(d))
    s3(1)
    s3(2)
    s1(0, 0)
    s1(0, 1)
    s3(3)
    for l in (1, 2, 3):
        yclose(l)
    mine = yclose(0)
    for d in range(1, 16):
        net.recv(("lz", d), lz.at[lax.rem(here + 16 - d, 16)], zdev(d))
    ln[0] = jnp.sum(lz[...], axis=0)
    share(0, axes[0])
    s3(0)
    shared(0, axes[0])
    share(1, axes[1])
    for l in (1, 2, 3):
        net.recv(("l", l), wl0.at[l], p.dev(dl=l))
    grad = (mine + f(wl0.at[1])) + (f(wl0.at[2]) + f(wl0.at[3]))
    old = fv_ref[...]
    out_ref[pl.ds(256, 128)] = old - STEP * (grad + RIDGE * old)
    shared(1, axes[1])
    loss_ref[0, 0] = jnp.sum(ln[2]) * (1.0 / entries)
    for j in (1, 2, 3):
        for h in range(len(halves[j])):
            net.recv(("z", j, h), zb.at[j, cut(j, h)], p.dev(dz=DZ[j]))
    grad = (w0[...] + f(zb.at[1])) + (f(zb.at[2]) + f(zb.at[3]))
    old = fu_ref[...]
    out_ref[pl.ds(0, 256)] = old - STEP * (grad + RIDGE * old)
    net.finish()


def vmem():
    return pl.BlockSpec(memory_space=pltpu.VMEM)


def per_device(factor_u, factor_v, values, mask_words, tile_cols):
    entries = lax.axis_size("rows") * lax.axis_size("cols") * 32 * 256 * 256
    far = pl.BlockSpec(memory_space=pltpu.HBM)
    near = pl.BlockSpec(memory_space=pltpu.SMEM)

    def low(*shape):
        return pltpu.VMEM(shape, BF16)

    def full(*shape):
        return pltpu.VMEM(shape, F32)

    out, loss = pl.pallas_call(
        lambda *refs: fused_kernel(entries, *refs),
        out_shape=(jax.ShapeDtypeStruct((384, 128), F32), jax.ShapeDtypeStruct((1, 1), F32)),
        in_specs=[far, far, far, far, near],
        out_specs=(vmem(), near),
        scratch_shapes=[
            full(256, 128),
            full(128, 128),
            low(32, 256, 128),
            low(16, 128, 128),
            low(32, 256, 256),
            pltpu.VMEM((32, 16, 256), jnp.int32),
            pltpu.SMEM((40,), jnp.int32),
            full(32, 128, 256),
            low(4, 2, 4, 256, 128),
            low(16, 128, 128),
            full(1, 128),
            low(4, 4, 256, 128),
            low(4, 4, 256, 128),
            low(4, 4, 256, 128),
            low(4, 256, 128),
            full(256, 128),
            low(4, 256, 128),
            low(4, 4, 128, 128),
            low(4, 128, 128),
            low(4, 128, 128),
            full(4, 4, 1, 128),
            full(1, 1, 128),
            full(5, 1, 128),
            full(16, 1, 128),
            full(1, 1, 128),
            pltpu.SemaphoreType.DMA((10,)),
            pltpu.SemaphoreType.DMA((N_COPIES,)),
            pltpu.SemaphoreType.DMA((N_COPIES,)),
        ],
        compiler_params=pltpu.CompilerParams(collective_id=0, has_side_effects=True),
        name="fused",
    )(factor_u[0], factor_v[0], values[0, 0], mask_words[0, 0], tile_cols[0, 0])
    def close(out_ref, u_hbm, v_hbm, sems):
        one = pltpu.make_async_copy(out_ref.at[pl.ds(0, 256)], u_hbm, sems.at[0])
        two = pltpu.make_async_copy(out_ref.at[pl.ds(256, 128)], v_hbm, sems.at[1])
        one.start()
        two.start()
        one.wait()
        two.wait()

    new_u, new_v = pl.pallas_call(
        close,
        out_shape=(jax.ShapeDtypeStruct((256, 128), F32), jax.ShapeDtypeStruct((128, 128), F32)),
        in_specs=[vmem()],
        out_specs=(far, far),
        scratch_shapes=[pltpu.SemaphoreType.DMA((2,))],
        name="close",
    )(out)
    return new_u[None], new_v[None], loss[0, 0]


def solution(mesh):
    return jax.shard_map(
        per_device,
        mesh=mesh,
        in_specs=(
            P("rows", "cols", None),
            P("cols", "rows", None),
            P("rows", "cols", None, None, None),
            P("rows", "cols", None, None, None),
            P("rows", "cols", None),
        ),
        out_specs=(P("rows", "cols", None), P("cols", "rows", None), P()),
        check_vma=False,
    )
```
